32 devices in a mesh: tm: 16 (over z, y, core), series: 2 (over x).
Axes of the slice: x: 2, y: 2, z: 4, core: 2. Of those that a mesh axis runs over, the one named last changes fastest.
Arguments:
- history: bfloat16 [4, 4096, 1024], P('series', 'tm'), may hold values from -36 to 36
- lengths: int32 [4], P('series'), may hold values from 512 to 4096
- head_window: int32 [16], replicated, may hold values from 32 to 512, as said below
- input_proj: bfloat16 [1024, 3072], replicated
- output_proj: bfloat16 [1024, 1024], replicated, may hold values from -0.1875 to 0.1875
- mixer_down: bfloat16 [1024, 512], replicated, may hold values from -0.1875 to 0.1875
- mixer_up: bfloat16 [512, 1024], replicated, may hold values from -0.25 to 0.25
- series_mix: bfloat16 [4, 4], replicated, may hold values from -3 to 3
Outputs:
- layer_out: bfloat16 [4, 4096, 1024], P('series', 'tm')
The draws below stay inside these ranges and needn't reach their ends.
Inputs may be any that keep to these rules, and one draw needn't show every extreme that they name: `head_window`: some head has exactly 512.
All inputs are finite; a program needn't handle non-finite values.
Results may differ from the reference program's by a relative error of at most 0.0065.
Values may be sent and summed in bfloat16 or wider, within the bound.
A program may use at most 128 MiB of HBM per device.

```python
import jax
import jax.numpy as jnp
from jax import lax

D = 1024
HEADS = 16
MIX_WIDTH = 512
WINDOW = 512
PATCHES = 4096
SERIES = 4


def draw_history(key, part):
    base = jnp.clip(jax.random.normal(key, (SERIES, PATCHES, D), jnp.float32), -6.0, 6.0)
    return base.astype(jnp.bfloat16)


def draw_head_window(key, part):
    windows = jax.random.randint(key, (HEADS,), max(WINDOW // 16, 1), WINDOW + 1, dtype=jnp.int32)
    chosen = jax.random.randint(jax.random.fold_in(key, 7), (), 0, HEADS, dtype=jnp.int32)
    return windows.at[chosen].set(WINDOW)


def draw_input_proj(key, part):
    first = jax.random.normal(jax.random.fold_in(key, 1), (D, D), jnp.float32)
    second = jax.random.normal(jax.random.fold_in(key, 2), (D, D), jnp.float32)
    third = jax.random.normal(jax.random.fold_in(key, 3), (D, D), jnp.float32)
    keyed = 0.6 * first + 0.8 * second
    return (jnp.concatenate([first, keyed, third], axis=1) * D ** (-0.5)).astype(jnp.bfloat16)


def with_ends(result, own_key, smallest, high):
    longest = result.shape.index(max(result.shape))
    spots = []
    for shift in (0, 1):
        where = [jax.random.randint(jax.random.fold_in(own_key, axis), (), 0, length) for axis, length in enumerate(result.shape)]
        where[longest] = (where[longest] + shift) % result.shape[longest]
        spots.append(tuple(where))
    return result.at[spots[0]].set(smallest).at[spots[1]].set(high)


def normal_values(key, shape, deviation, limit, kind=jnp.bfloat16):
    result = deviation * jax.random.normal(key, shape, jnp.float32)
    return jnp.clip(result, min=-limit, max=limit).astype(kind)


def setup_inputs(seed: int = 0) -> dict:
    key_list = jax.random.split(jax.random.key(seed), 9)
    return {
        "history": draw_history(jax.random.fold_in(key_list[8], 71), 0),
        "lengths": with_ends(jax.random.randint(key_list[1], (SERIES,), WINDOW, PATCHES + 1), jax.random.fold_in(key_list[1], 1), WINDOW, PATCHES).astype(jnp.int32),
        "head_window": draw_head_window(jax.random.fold_in(key_list[8], 71), 0),
        "input_proj": draw_input_proj(jax.random.fold_in(key_list[8], 71), 0),
        "output_proj": normal_values(key_list[4], (D, D), D ** -0.5, 0.1875),
        "mixer_down": normal_values(key_list[5], (D, MIX_WIDTH), D ** -0.5, 0.1875),
        "mixer_up": normal_values(key_list[6], (MIX_WIDTH, D), MIX_WIDTH ** -0.5, 0.25),
        "series_mix": normal_values(key_list[7], (SERIES, SERIES), SERIES ** -0.5, 3.0),
    }


def attend(queries, keys_values, length, head_window, query_first, key_first):
    query_rows = queries.shape[0]
    key_rows = keys_values.shape[0]
    head_size = D // HEADS
    query_heads = queries.astype(jnp.float32).reshape(query_rows, HEADS, head_size)
    key_heads = keys_values[:, :D].astype(jnp.float32).reshape(key_rows, HEADS, head_size)
    value_heads = keys_values[:, D:].astype(jnp.float32).reshape(key_rows, HEADS, head_size)
    scores = jnp.einsum("qhd,khd->hqk", query_heads, key_heads) * (head_size ** -0.5)
    query_pos = query_first + jnp.arange(query_rows, dtype=jnp.int32)
    key_pos = key_first + jnp.arange(key_rows, dtype=jnp.int32)
    key_valid = (key_pos >= PATCHES - length) & (key_pos < PATCHES)
    distance = jnp.abs(query_pos[:, None] - key_pos[None, :])
    allowed = (distance[None, :, :] <= head_window[:, None, None]) & key_valid[None, None, :]
    scores = jnp.where(allowed, scores, -1e30)
    largest = jnp.max(scores, axis=-1, keepdims=True)
    weights = jnp.exp(scores - largest)
    totals = jnp.sum(weights, axis=-1)
    probabilities = weights.astype(jnp.bfloat16).astype(jnp.float32)
    combined = jnp.einsum("hqk,khd->qhd", probabilities, value_heads) / jnp.transpose(totals)[:, :, None]
    combined = combined.reshape(query_rows, D)
    query_valid = query_pos >= PATCHES - length
    return jnp.where(query_valid[:, None], combined, 0.0).astype(jnp.bfloat16)


def reference(history, lengths, head_window, input_proj, output_proj, mixer_down, mixer_up, series_mix):
    block_rows = min(512, PATCHES)
    block_count = PATCHES // block_rows

    def per_series(inputs):
        series_rows, length = inputs
        packed = jnp.dot(series_rows, input_proj, preferred_element_type=jnp.float32).astype(jnp.bfloat16)
        queries = packed[:, :D]
        padded = jnp.pad(packed[:, D:], ((WINDOW, WINDOW), (0, 0)))

        def per_block(block_index):
            first_row = (block_index * block_rows).astype(jnp.int32)
            query_block = lax.dynamic_slice_in_dim(queries, first_row, block_rows, 0)
            key_block = lax.dynamic_slice_in_dim(padded, first_row, block_rows + 2 * WINDOW, 0)
            return attend(query_block, key_block, length, head_window, first_row, first_row - WINDOW)

        attended = lax.map(per_block, jnp.arange(block_count, dtype=jnp.int32)).reshape(PATCHES, D)
        hidden = (series_rows.astype(jnp.float32) + jnp.dot(attended, output_proj, preferred_element_type=jnp.float32)).astype(jnp.bfloat16)
        branch = jnp.dot(hidden, mixer_down, preferred_element_type=jnp.float32).astype(jnp.bfloat16)
        return hidden, branch

    hidden, branch = lax.map(per_series, (history, lengths))
    combined = jnp.einsum("ab,bpc->apc", series_mix.astype(jnp.float32), branch.astype(jnp.float32)).astype(jnp.bfloat16)
    update = jnp.dot(combined.reshape(SERIES * PATCHES, MIX_WIDTH), mixer_up, preferred_element_type=jnp.float32)
    return (hidden.astype(jnp.float32) + update.reshape(SERIES, PATCHES, D)).astype(jnp.bfloat16)
```

```python
import functools

import jax
import jax.numpy as jnp
from jax import lax
from jax.experimental import pallas as pl
from jax.experimental.pallas import tpu as pltpu
from jax.sharding import PartitionSpec as P

HEADS = 16
WINDOW = 512
BLOCK = 128
MASKED = -1e30
PIECES = 4
MESH = pl.DeviceIdType.MESH


def exchange_kernel(
    history_ref, weight_hbm, queries_ref, context_ref,
    halo, weight, weight_sem, partner_send, partner_recv, y_send, y_recv,
    z_send, z_recv, x_send, x_recv, *, scale,
):
    series, rows, width = history_ref.shape
    tiles = 6
    tile = weight.shape[1] // tiles
    piece = rows // PIECES
    me = lax.axis_index("tm")
    count = lax.axis_size("tm")
    core = me % 2
    side = (me // 2) % 2
    partner = me + 1 - 2 * core
    across = me + 2 - 4 * side
    onward = me + 4 - 8 * side
    origin = me - 4 + 8 * side
    has_onward = (onward >= 0) & (onward < count)
    has_origin = (origin >= 0) & (origin < count)

    loads = [
        pltpu.make_async_copy(
            weight_hbm.at[:, pl.ds(t * tile, tile)],
            weight.at[:, pl.ds(t * tile, tile)],
            weight_sem.at[t],
        )
        for t in range(tiles)
    ]
    for load in loads[2:] + loads[:2]:
        load.start()

    barrier = pltpu.get_barrier_semaphore()
    for other in (partner, across):
        pl.semaphore_signal(barrier, inc=1, device_id={"tm": other}, device_id_type=MESH)
    for other, exists in ((onward, has_onward), (origin, has_origin)):
        @pl.when(exists)
        def _():
            pl.semaphore_signal(barrier, inc=1, device_id={"tm": other}, device_id_type=MESH)
    peers = 2 + jnp.where(has_onward, 1, 0) + jnp.where(has_origin, 1, 0)
    pl.semaphore_wait(barrier, peers)

    def remote(source, target, send, recv, device):
        return pltpu.make_async_remote_copy(
            src_ref=source, dst_ref=target, send_sem=send, recv_sem=recv,
            device_id={"tm": device}, device_id_type=MESH,
        )

    def y_copy(s, r):
        part = pl.ds(r * piece, piece)
        return remote(
            history_ref.at[s, part, :], halo.at[1, s, part, :],
            y_send.at[s, r], y_recv.at[s, r], across,
        )

    def z_copy(s, r):
        part = pl.ds(r * piece, piece)
        return remote(
            halo.at[1, s, part, :], halo.at[2, s, part, :],
            z_send.at[s, r], z_recv.at[s, r], onward,
        )

    def partner_copy(s):
        return remote(
            history_ref.at[s], halo.at[0, s], partner_send.at[s], partner_recv.at[s], partner
        )

    def x_copy(s, role):
        return remote(halo.at[role, s], halo.at[3, s], x_send.at[s], x_recv.at[s], partner)

    for s in range(series):
        for r in range(PIECES):
            y_copy(s, r).start()
        partner_copy(s).start()

    @pl.when(jnp.logical_not(has_origin))
    def _():
        halo[2] = jnp.zeros(halo.shape[1:], halo.dtype)

    def project(source, s, slot):
        first = pl.multiple_of(slot * rows, rows)

        def body(t, _):
            column = pl.multiple_of(t * tile, tile)
            out = jnp.dot(
                source[...], weight[:, pl.ds(width + column, tile)],
                preferred_element_type=jnp.float32,
            )
            context_ref[s, pl.ds(first, rows), pl.ds(column, tile)] = out.astype(jnp.bfloat16)
            return 0

        lax.fori_loop(0, 2 * width // tile, body, 0)

    def project_queries(s):
        def body(t, _):
            column = pl.multiple_of(t * tile, tile)
            out = jnp.dot(
                history_ref[s], weight[:, pl.ds(column, tile)],
                preferred_element_type=jnp.float32,
            )
            queries_ref[s, :, pl.ds(column, tile)] = out.astype(jnp.bfloat16) * scale
            return 0

        lax.fori_loop(0, width // tile, body, 0)

    def relay(s, r):
        y_copy(s, r).wait_recv()

        @pl.when(has_onward)
        def _():
            z_copy(s, r).start()

    near = core == side
    slot_partner = 3 - 2 * core
    slot_a = 4 - 4 * side
    slot_b = 4 * side
    slot_x = 1 + 2 * core

    def finish_a(s):
        @pl.when(near)
        def _():
            x_copy(s, 1).start()
        project(halo.at[1, s], s, slot_a)

    def finish_b(s):
        @pl.when(has_origin)
        def _():
            for r in range(PIECES):
                z_copy(s, r).wait_recv()

        @pl.when(jnp.logical_not(near))
        def _():
            x_copy(s, 2).start()
        project(halo.at[2, s], s, slot_b)

    def finish_x(s):
        x_copy(s, 1).wait_recv()
        project(halo.at[3, s], s, slot_x)

    for load in loads[2:]:
        load.wait()
    project(history_ref.at[0], 0, 2)
    for load in loads[:2]:
        load.wait()
    project_queries(0)
    relay(0, 0)
    project(history_ref.at[1], 1, 2)
    project_queries(1)
    relay(0, 1)
    for s in range(series):
        partner_copy(s).wait_recv()
        project(halo.at[0, s], s, slot_partner)
    relay(0, 2)
    relay(0, 3)
    finish_a(0)
    relay(1, 0)
    finish_b(0)
    relay(1, 1)
    finish_x(0)
    relay(1, 2)
    relay(1, 3)
    finish_a(1)
    finish_b(1)
    finish_x(1)

    for s in range(series):
        partner_copy(s).wait_send()
        x_copy(s, 1).wait_send()
        for r in range(PIECES):
            y_copy(s, r).wait_send()

    @pl.when(has_onward)
    def _():
        for s in range(series):
            for r in range(PIECES):
                z_copy(s, r).wait_send()


def attention_kernel(lengths_ref, window_ref, queries_ref, context_ref, out_ref, bias_ref, *, hops):
    series, rows, width = queries_ref.shape
    keys = context_ref.shape[1]
    head_size = width // HEADS
    pairs = width // BLOCK
    reach = WINDOW // BLOCK
    me = lax.axis_index("tm")
    patches = rows * lax.axis_size("tm")
    first = me * rows - hops * rows
    center = hops * rows // BLOCK
    key_pos = first + lax.broadcasted_iota(jnp.int32, (1, keys), 1)
    query_pos = me * rows + lax.broadcasted_iota(jnp.int32, (rows, BLOCK), 0)

    for s in range(series):
        start = patches - lengths_ref[s]
        bias_ref[s] = jnp.where((key_pos >= start) & (key_pos < patches), 0.0, MASKED)

    def one_head(s, pair, half, steps, window):
        column = pl.multiple_of(pair * BLOCK, BLOCK)
        lane = lax.broadcasted_iota(jnp.int32, (BLOCK, BLOCK), 1)
        tilt = lane - lax.broadcasted_iota(jnp.int32, (BLOCK, BLOCK), 0)
        mine = (lane // head_size) == half
        span = (2 * steps + 1) * BLOCK
        for part in range(rows // BLOCK):
            low = (center + part - steps) * BLOCK
            q = queries_ref[s, part * BLOCK : (part + 1) * BLOCK, pl.ds(column, BLOCK)]
            q = jnp.where(mine, q, jnp.zeros_like(q))
            k = context_ref[s, low : low + span, pl.ds(column, BLOCK)]
            scores = lax.dot_general(
                q, k, (((1,), (1,)), ((), ())), preferred_element_type=jnp.float32
            )
            chunks = []
            for o in range(-steps, steps + 1):
                at = (o + steps) * BLOCK
                chunk = scores[:, at : at + BLOCK] + bias_ref[s, :, low + at : low + at + BLOCK]
                if abs(o) >= steps - 1:
                    if o <= 0:
                        chunk = jnp.where(tilt >= -(window + o * BLOCK), chunk, MASKED)
                    if o >= 0:
                        chunk = jnp.where(tilt <= window - o * BLOCK, chunk, MASKED)
                chunks.append(chunk)
            top = chunks[0]
            for chunk in chunks[1:]:
                top = jnp.maximum(top, chunk)
            top = jnp.max(top, axis=1, keepdims=True)
            weights = jnp.concatenate(
                [jnp.exp(chunk - top).astype(jnp.bfloat16) for chunk in chunks], axis=1
            )
            v = context_ref[s, low : low + span, pl.ds(width + column, BLOCK)]
            v = jnp.concatenate([v, jnp.ones((span, BLOCK), jnp.bfloat16)], axis=1)
            both = jnp.dot(weights, v, preferred_element_type=jnp.float32)
            result = both[:, :BLOCK] / both[:, BLOCK:]
            here = query_pos[part * BLOCK : (part + 1) * BLOCK]
            result = jnp.where(here >= patches - lengths_ref[s], result, 0.0).astype(jnp.bfloat16)
            place = (s, slice(part * BLOCK, (part + 1) * BLOCK), pl.ds(column, BLOCK))
            if half:
                result = jnp.where(mine, result, out_ref[place])
            out_ref[place] = result

    def body(index, _):
        s = index // pairs
        pair = index % pairs
        for half in range(BLOCK // head_size):
            window = window_ref[pair * (BLOCK // head_size) + half]
            needed = (window + BLOCK - 1) // BLOCK
            for steps in range(1, reach + 1):
                @pl.when(needed == steps)
                def _():
                    one_head(s, pair, half, steps, window)
        return 0

    lax.fori_loop(0, series * pairs, body, 0)


def on_device(
    history, lengths, head_window, input_proj, output_proj, mixer_down, mixer_up, series_mix
):
    series, rows, width = history.shape
    hops = -(-WINDOW // rows)
    keys = (2 * hops + 1) * rows
    head_size = width // HEADS
    vmem = pl.BlockSpec(memory_space=pltpu.VMEM)
    smem = pl.BlockSpec(memory_space=pltpu.SMEM)
    dma = pltpu.SemaphoreType.DMA
    queries, context = pl.pallas_call(
        functools.partial(exchange_kernel, scale=head_size ** (-0.5)),
        out_shape=(
            jax.ShapeDtypeStruct((series, rows, width), jnp.bfloat16),
            jax.ShapeDtypeStruct((series, keys, 2 * width), jnp.bfloat16),
        ),
        in_specs=[vmem, pl.BlockSpec(memory_space=pltpu.HBM)],
        out_specs=(vmem, vmem),
        scratch_shapes=[
            pltpu.VMEM((4, series, rows, width), jnp.bfloat16),
            pltpu.VMEM(input_proj.shape, jnp.bfloat16),
            dma((6,)),
            dma((series,)),
            dma((series,)),
            dma((series, PIECES)),
            dma((series, PIECES)),
            dma((series, PIECES)),
            dma((series, PIECES)),
            dma((series,)),
            dma((series,)),
        ],
        compiler_params=pltpu.CompilerParams(
            collective_id=0, has_side_effects=True, vmem_limit_bytes=32 * 1024 * 1024
        ),
    )(history, input_proj)
    attended = pl.pallas_call(
        functools.partial(attention_kernel, hops=hops),
        out_shape=jax.ShapeDtypeStruct((series, rows, width), jnp.bfloat16),
        in_specs=[smem, smem, vmem, vmem],
        out_specs=vmem,
        scratch_shapes=[pltpu.VMEM((series, 1, keys), jnp.float32)],
        compiler_params=pltpu.CompilerParams(vmem_limit_bytes=32 * 1024 * 1024),
    )(lengths, head_window, queries, context)
    hidden = (
        history.astype(jnp.float32)
        + jnp.einsum("spd,de->spe", attended, output_proj, preferred_element_type=jnp.float32)
    ).astype(jnp.bfloat16)
    branch = jnp.einsum(
        "spd,dc->spc", hidden, mixer_down, preferred_element_type=jnp.float32
    ).astype(jnp.bfloat16)
    groups = lax.axis_size("series")
    group = lax.axis_index("series")
    own_rows = lax.dynamic_slice_in_dim(series_mix, group * series, series, 0)

    def mixed(part, source):
        share = lax.dynamic_slice_in_dim(own_rows, source * series, series, 1)
        return jnp.einsum("ab,bpc->apc", share, part, preferred_element_type=jnp.float32)

    combined = mixed(branch, group)
    for offset in range(1, groups):
        route = [(i, (i + offset) % groups) for i in range(groups)]
        part = lax.ppermute(branch, "series", route)
        combined = combined + mixed(part, (group - offset) % groups)
    combined = combined.astype(jnp.bfloat16)
    update = jnp.einsum("spc,cd->spd", combined, mixer_up, preferred_element_type=jnp.float32)
    return (hidden.astype(jnp.float32) + update).astype(jnp.bfloat16)


def solution(mesh):
    in_specs = (P("series", "tm", None), P("series"), P(), P(), P(), P(), P(), P())
    out_specs = P("series", "tm", None)
    return jax.shard_map(
        on_device, mesh=mesh, in_specs=in_specs, out_specs=out_specs, check_vma=False
    )
```

```python
import functools

import jax
import jax.numpy as jnp
from jax import lax
from jax.experimental import pallas as pl
from jax.experimental.pallas import tpu as pltpu
from jax.sharding import PartitionSpec as P

HEADS = 16
WINDOW = 512
BLOCK = 128
MASKED = -1e30
LIMIT = 46
PIECES = 4
MESH = pl.DeviceIdType.MESH


def exchange_kernel(
    history_ref, weight_hbm, queries_ref, context_ref,
    halo, weight, weight_sem, partner_send, partner_recv, y_send, y_recv,
    z_send, z_recv, x_send, x_recv, *, scale,
):
    series, rows, width = history_ref.shape
    tiles = 6
    tile = weight.shape[1] // tiles
    piece = rows // PIECES
    me = lax.axis_index("tm")
    count = lax.axis_size("tm")
    core = me % 2
    side = (me // 2) % 2
    partner = me + 1 - 2 * core
    across = me + 2 - 4 * side
    onward = me + 4 - 8 * side
    origin = me - 4 + 8 * side
    has_onward = (onward >= 0) & (onward < count)
    has_origin = (origin >= 0) & (origin < count)

    loads = [
        pltpu.make_async_copy(
            weight_hbm.at[:, pl.ds(t * tile, tile)],
            weight.at[:, pl.ds(t * tile, tile)],
            weight_sem.at[t],
        )
        for t in range(tiles)
    ]
    for load in loads[2:] + loads[:2]:
        load.start()

    barrier = pltpu.get_barrier_semaphore()
    for other in (partner, across):
        pl.semaphore_signal(barrier, inc=1, device_id={"tm": other}, device_id_type=MESH)
    for other, exists in ((onward, has_onward), (origin, has_origin)):
        @pl.when(exists)
        def _():
            pl.semaphore_signal(barrier, inc=1, device_id={"tm": other}, device_id_type=MESH)
    peers = 2 + jnp.where(has_onward, 1, 0) + jnp.where(has_origin, 1, 0)
    pl.semaphore_wait(barrier, peers)

    def remote(source, target, send, recv, device):
        return pltpu.make_async_remote_copy(
            src_ref=source, dst_ref=target, send_sem=send, recv_sem=recv,
            device_id={"tm": device}, device_id_type=MESH,
        )

    def y_copy(s, r):
        part = pl.ds(r * piece, piece)
        return remote(
            history_ref.at[s, part, :], halo.at[1, s, part, :],
            y_send.at[s, r], y_recv.at[s, r], across,
        )

    def z_copy(s, r):
        part = pl.ds(r * piece, piece)
        return remote(
            halo.at[1, s, part, :], halo.at[2, s, part, :],
            z_send.at[s, r], z_recv.at[s, r], onward,
        )

    def partner_copy(s):
        return remote(
            history_ref.at[s], halo.at[0, s], partner_send.at[s], partner_recv.at[s], partner
        )

    unit = rows // 2

    def x_copy(s, h, role):
        part = pl.ds(h * unit, unit)
        return remote(
            halo.at[role, s, part, :], halo.at[3, s, part, :],
            x_send.at[s, h], x_recv.at[s, h], partner,
        )

    for s in range(series):
        for r in range(PIECES):
            y_copy(s, r).start()
        partner_copy(s).start()

    @pl.when(jnp.logical_not(has_origin))
    def _():
        halo[2] = jnp.zeros(halo.shape[1:], halo.dtype)

    def project(source, s, slot, h=0):
        size = source.shape[0]
        first = pl.multiple_of(slot * rows + h * unit, unit)

        def body(t, _):
            column = pl.multiple_of(t * tile, tile)
            out = jnp.dot(
                source[...], weight[:, pl.ds(width + column, tile)],
                preferred_element_type=jnp.float32,
            )
            context_ref[s, pl.ds(first, size), pl.ds(column, tile)] = out.astype(jnp.bfloat16)
            return 0

        lax.fori_loop(0, 2 * width // tile, body, 0)

    def project_queries(s):
        def body(t, _):
            column = pl.multiple_of(t * tile, tile)
            out = jnp.dot(
                history_ref[s], weight[:, pl.ds(column, tile)],
                preferred_element_type=jnp.float32,
            )
            queries_ref[s, :, pl.ds(column, tile)] = out.astype(jnp.bfloat16) * scale
            return 0

        lax.fori_loop(0, width // tile, body, 0)

    def relay(s, r):
        y_copy(s, r).wait_recv()

        @pl.when(has_onward)
        def _():
            z_copy(s, r).start()

    near = core == side
    slot_partner = 3 - 2 * core
    slot_a = 4 - 4 * side
    slot_b = 4 * side
    slot_x = 1 + 2 * core

    def half_of(role, s, h):
        return halo.at[role, s, pl.ds(h * unit, unit), :]

    def finish_a(s, h):
        @pl.when(near)
        def _():
            x_copy(s, h, 1).start()
        project(half_of(1, s, h), s, slot_a, h)

    def finish_b(s, h):
        @pl.when(has_origin)
        def _():
            for r in range(h * PIECES // 2, (h + 1) * PIECES // 2):
                z_copy(s, r).wait_recv()

        @pl.when(jnp.logical_not(near))
        def _():
            x_copy(s, h, 2).start()
        project(half_of(2, s, h), s, slot_b, h)

    def finish_x(s, h):
        x_copy(s, h, 1).wait_recv()
        project(half_of(3, s, h), s, slot_x, h)

    for load in loads[2:]:
        load.wait()
    project(history_ref.at[0], 0, 2)
    for load in loads[:2]:
        load.wait()
    project_queries(0)
    relay(0, 0)
    project(history_ref.at[1], 1, 2)
    project_queries(1)
    relay(0, 1)
    for s in range(series):
        partner_copy(s).wait_recv()
        project(halo.at[0, s], s, slot_partner)
    finish_a(0, 0)
    relay(0, 2)
    relay(0, 3)
    finish_b(0, 0)
    finish_x(0, 0)
    finish_a(0, 1)
    relay(1, 0)
    finish_b(0, 1)
    finish_x(0, 1)
    relay(1, 1)
    finish_a(1, 0)
    relay(1, 2)
    finish_b(1, 0)
    finish_x(1, 0)
    relay(1, 3)
    finish_a(1, 1)
    finish_b(1, 1)
    finish_x(1, 1)

    for s in range(series):
        partner_copy(s).wait_send()
        for h in range(2):
            x_copy(s, h, 1).wait_send()
        for r in range(PIECES):
            y_copy(s, r).wait_send()

    @pl.when(has_onward)
    def _():
        for s in range(series):
            for r in range(PIECES):
                z_copy(s, r).wait_send()


def attention_kernel(
    lengths_ref, window_ref, queries_ref, context_ref, out_ref, bias_ref, weights_ref, *, s, hops
):
    rows, width = out_ref.shape
    keys = context_ref.shape[1]
    head_size = width // HEADS
    sharing = BLOCK // head_size
    pairs = width // BLOCK
    reach = WINDOW // BLOCK
    parts = rows // BLOCK
    me = lax.axis_index("tm")
    patches = rows * lax.axis_size("tm")
    first = me * rows - hops * rows
    center = hops * rows // BLOCK
    start = patches - lengths_ref[s]
    key_pos = first + lax.broadcasted_iota(jnp.int32, (1, keys), 1)
    bias_ref[...] = jnp.where((key_pos >= start) & (key_pos < patches), 0.0, MASKED)
    query_valid = me * rows + lax.broadcasted_iota(jnp.int32, (rows, BLOCK), 0) >= start
    lane = lax.broadcasted_iota(jnp.int32, (rows, BLOCK), 1)
    tilt = lax.broadcasted_iota(jnp.int32, (BLOCK, BLOCK), 1) - lax.broadcasted_iota(
        jnp.int32, (BLOCK, BLOCK), 0
    )

    def group(pair, steps):
        column = pl.multiple_of(pair * BLOCK, BLOCK)
        low = (center - steps) * BLOCK
        spots = 2 * steps + parts
        span = spots * BLOCK
        q = queries_ref[s, :, pl.ds(column, BLOCK)]
        q = jnp.concatenate(
            [jnp.where(lane // head_size == h, q, jnp.zeros_like(q)) for h in range(sharing)],
            axis=0,
        )
        k = context_ref[s, low : low + span, pl.ds(column, BLOCK)]
        scores = lax.dot_general(
            q, k, (((1,), (1,)), ((), ())), preferred_element_type=jnp.float32
        )
        for h in range(sharing):
            window = window_ref[pair * sharing + h]
            for part in range(parts):
                top_row = (h * parts + part) * BLOCK
                chunks = {}
                for spot in range(part, part + 2 * steps + 1):
                    o = spot - part - steps
                    at = spot * BLOCK
                    chunk = (
                        scores[top_row : top_row + BLOCK, at : at + BLOCK]
                        + bias_ref[:, low + at : low + at + BLOCK]
                    )
                    if o <= 0:
                        chunk = jnp.where(tilt >= -(window + o * BLOCK), chunk, MASKED)
                    if o >= 0:
                        chunk = jnp.where(tilt <= window - o * BLOCK, chunk, MASKED)
                    chunks[spot] = chunk
                top = functools.reduce(jnp.maximum, chunks.values())
                top = jnp.max(top, axis=1, keepdims=True)
                for spot in range(spots):
                    if spot in chunks:
                        value = jnp.exp(chunks[spot] - top).astype(jnp.bfloat16)
                    else:
                        value = jnp.zeros((BLOCK, BLOCK), jnp.bfloat16)
                    weights_ref[
                        top_row : top_row + BLOCK, spot * BLOCK : (spot + 1) * BLOCK
                    ] = value
        v = context_ref[s, low : low + span, pl.ds(width + column, BLOCK)]
        v = jnp.concatenate([v, jnp.ones((span, BLOCK), jnp.bfloat16)], axis=1)
        both = jnp.dot(weights_ref[:, :span], v, preferred_element_type=jnp.float32)
        both = both[:, :BLOCK] / both[:, BLOCK:]
        result = both[:rows]
        for h in range(1, sharing):
            result = jnp.where(lane // head_size == h, both[h * rows : (h + 1) * rows], result)
        out_ref[:, pl.ds(column, BLOCK)] = jnp.where(query_valid, result, 0.0).astype(jnp.bfloat16)

    def body(pair, _):
        window = window_ref[pair * sharing]
        for h in range(1, sharing):
            window = jnp.maximum(window, window_ref[pair * sharing + h])
        needed = (window + BLOCK - 1) // BLOCK
        for steps in range(1, reach + 1):
            @pl.when(needed == steps)
            def _():
                group(pair, steps)
        return 0

    lax.fori_loop(0, pairs, body, 0)


def on_device(
    history, lengths, head_window, input_proj, output_proj, mixer_down, mixer_up, series_mix
):
    series, rows, width = history.shape
    hops = -(-WINDOW // rows)
    keys = (2 * hops + 1) * rows
    head_size = width // HEADS
    vmem = pl.BlockSpec(memory_space=pltpu.VMEM)
    smem = pl.BlockSpec(memory_space=pltpu.SMEM)
    dma = pltpu.SemaphoreType.DMA
    queries, context = pl.pallas_call(
        functools.partial(exchange_kernel, scale=head_size ** (-0.5)),
        out_shape=(
            pltpu.VMEM((series, rows, width), jnp.bfloat16),
            pltpu.VMEM((series, keys, 2 * width), jnp.bfloat16),
        ),
        in_specs=[vmem, pl.BlockSpec(memory_space=pltpu.HBM)],
        out_specs=(vmem, vmem),
        scratch_shapes=[
            pltpu.VMEM((4, series, rows, width), jnp.bfloat16),
            pltpu.VMEM(input_proj.shape, jnp.bfloat16),
            dma((6,)),
            dma((series,)),
            dma((series,)),
            dma((series, PIECES)),
            dma((series, PIECES)),
            dma((series, PIECES)),
            dma((series, PIECES)),
            dma((series, 2)),
            dma((series, 2)),
        ],
        compiler_params=pltpu.CompilerParams(
            collective_id=0, has_side_effects=True, vmem_limit_bytes=LIMIT * 1024 * 1024
        ),
    )(history, input_proj)
    groups = lax.axis_size("series")
    group = lax.axis_index("series")
    mix = series_mix.astype(jnp.float32)
    hiddens = []
    combined = [0.0] * series
    for s in range(series):
        attended = pl.pallas_call(
            functools.partial(attention_kernel, s=s, hops=hops),
            out_shape=jax.ShapeDtypeStruct((rows, width), jnp.bfloat16),
            in_specs=[smem, smem, vmem, vmem],
            out_specs=vmem,
            scratch_shapes=[
                pltpu.VMEM((1, keys), jnp.float32),
                pltpu.VMEM((rows * BLOCK // head_size, keys), jnp.bfloat16),
            ],
            compiler_params=pltpu.CompilerParams(vmem_limit_bytes=32 * 1024 * 1024),
            cost_estimate=pl.CostEstimate(
                flops=8 * rows * keys * width, bytes_accessed=0, transcendentals=0
            ),
        )(lengths, head_window, queries, context)
        hidden = (
            history[s].astype(jnp.float32)
            + jnp.dot(attended, output_proj, preferred_element_type=jnp.float32)
        ).astype(jnp.bfloat16)
        hiddens.append(hidden)
        branch = jnp.dot(hidden, mixer_down, preferred_element_type=jnp.float32).astype(
            jnp.bfloat16
        )
        for offset in range(groups):
            route = [(i, (i + offset) % groups) for i in range(groups)]
            part = lax.ppermute(branch, "series", route) if offset else branch
            column = (group - offset) % groups * series + s
            for a in range(series):
                weight = lax.dynamic_slice(mix, (group * series + a, column), (1, 1))
                combined[a] = combined[a] + weight * part.astype(jnp.float32)
    outs = []
    for a in range(series):
        update = jnp.dot(
            combined[a].astype(jnp.bfloat16), mixer_up, preferred_element_type=jnp.float32
        )
        outs.append((hiddens[a].astype(jnp.float32) + update).astype(jnp.bfloat16))
    return jnp.stack(outs)


def solution(mesh):
    in_specs = (P("series", "tm", None), P("series"), P(), P(), P(), P(), P(), P())
    out_specs = P("series", "tm", None)
    return jax.shard_map(
        on_device, mesh=mesh, in_specs=in_specs, out_specs=out_specs, check_vma=False
    )
```

```python
import functools

import jax
import jax.numpy as jnp
from jax import lax
from jax.experimental import pallas as pl
from jax.experimental.pallas import tpu as pltpu
from jax.sharding import PartitionSpec as P

HEADS = 16
WINDOW = 512
BLOCK = 128
MASKED = -1e30
LIMIT = 46
PIECES = 4
MESH = pl.DeviceIdType.MESH


def exchange_kernel(
    history_ref, weight_hbm, queries_ref, context_ref,
    halo, weight, weight_sem, partner_send, partner_recv, y_send, y_recv,
    z_send, z_recv, x_send, x_recv, *, scale,
):
    series, rows, width = history_ref.shape
    tiles = 6
    tile = weight.shape[1] // tiles
    piece = rows // PIECES
    me = lax.axis_index("tm")
    count = lax.axis_size("tm")
    core = me % 2
    side = (me // 2) % 2
    partner = me + 1 - 2 * core
    across = me + 2 - 4 * side
    onward = me + 4 - 8 * side
    origin = me - 4 + 8 * side
    has_onward = (onward >= 0) & (onward < count)
    has_origin = (origin >= 0) & (origin < count)

    loads = [
        pltpu.make_async_copy(
            weight_hbm.at[:, pl.ds(t * tile, tile)],
            weight.at[:, pl.ds(t * tile, tile)],
            weight_sem.at[t],
        )
        for t in range(tiles)
    ]
    for load in loads[2:] + loads[:2]:
        load.start()

    barrier = pltpu.get_barrier_semaphore()
    for other in (partner, across):
        pl.semaphore_signal(barrier, inc=1, device_id={"tm": other}, device_id_type=MESH)
    for other, exists in ((onward, has_onward), (origin, has_origin)):
        @pl.when(exists)
        def _():
            pl.semaphore_signal(barrier, inc=1, device_id={"tm": other}, device_id_type=MESH)
    peers = 2 + jnp.where(has_onward, 1, 0) + jnp.where(has_origin, 1, 0)
    pl.semaphore_wait(barrier, peers)

    def remote(source, target, send, recv, device):
        return pltpu.make_async_remote_copy(
            src_ref=source, dst_ref=target, send_sem=send, recv_sem=recv,
            device_id={"tm": device}, device_id_type=MESH,
        )

    def y_copy(s, r):
        part = pl.ds(r * piece, piece)
        return remote(
            history_ref.at[s, part, :], halo.at[1, s, part, :],
            y_send.at[s, r], y_recv.at[s, r], across,
        )

    def z_copy(s, r):
        part = pl.ds(r * piece, piece)
        return remote(
            halo.at[1, s, part, :], halo.at[2, s, part, :],
            z_send.at[s, r], z_recv.at[s, r], onward,
        )

    def partner_copy(s):
        return remote(
            history_ref.at[s], halo.at[0, s], partner_send.at[s], partner_recv.at[s], partner
        )

    unit = rows // 2

    def x_copy(s, h, role):
        part = pl.ds(h * unit, unit)
        return remote(
            halo.at[role, s, part, :], halo.at[3, s, part, :],
            x_send.at[s, h], x_recv.at[s, h], partner,
        )

    for s in range(series):
        for r in range(PIECES):
            y_copy(s, r).start()
        partner_copy(s).start()

    @pl.when(jnp.logical_not(has_origin))
    def _():
        halo[2] = jnp.zeros(halo.shape[1:], halo.dtype)

    def project(source, s, slot, h=0):
        size = source.shape[0]
        first = pl.multiple_of(slot * rows + h * unit, unit)

        def body(t, _):
            column = pl.multiple_of(t * tile, tile)
            out = jnp.dot(
                source[...], weight[:, pl.ds(width + column, tile)],
                preferred_element_type=jnp.float32,
            )
            context_ref[s, pl.ds(first, size), pl.ds(column, tile)] = out.astype(jnp.bfloat16)
            return 0

        lax.fori_loop(0, 2 * width // tile, body, 0)

    def project_queries(s):
        def body(t, _):
            column = pl.multiple_of(t * tile, tile)
            out = jnp.dot(
                history_ref[s], weight[:, pl.ds(column, tile)],
                preferred_element_type=jnp.float32,
            )
            queries_ref[s, :, pl.ds(column, tile)] = out.astype(jnp.bfloat16) * scale
            return 0

        lax.fori_loop(0, width // tile, body, 0)

    def relay(s, r):
        y_copy(s, r).wait_recv()

        @pl.when(has_onward)
        def _():
            z_copy(s, r).start()

    near = core == side
    slot_partner = 3 - 2 * core
    slot_a = 4 - 4 * side
    slot_b = 4 * side
    slot_x = 1 + 2 * core

    def half_of(role, s, h):
        return halo.at[role, s, pl.ds(h * unit, unit), :]

    def finish_a(s, h):
        @pl.when(near)
        def _():
            x_copy(s, h, 1).start()
        project(half_of(1, s, h), s, slot_a, h)

    def finish_b(s, h):
        @pl.when(has_origin)
        def _():
            for r in range(h * PIECES // 2, (h + 1) * PIECES // 2):
                z_copy(s, r).wait_recv()

        @pl.when(jnp.logical_not(near))
        def _():
            x_copy(s, h, 2).start()
        project(half_of(2, s, h), s, slot_b, h)

    def finish_x(s, h):
        x_copy(s, h, 1).wait_recv()
        project(half_of(3, s, h), s, slot_x, h)

    for load in loads[2:]:
        load.wait()
    project(history_ref.at[0], 0, 2)
    for load in loads[:2]:
        load.wait()
    project_queries(0)
    relay(0, 0)
    project(history_ref.at[1], 1, 2)
    project_queries(1)
    relay(0, 1)
    for s in range(series):
        partner_copy(s).wait_recv()
        project(halo.at[0, s], s, slot_partner)
    finish_a(0, 0)
    relay(0, 2)
    relay(0, 3)
    finish_b(0, 0)
    finish_x(0, 0)
    finish_a(0, 1)
    relay(1, 0)
    finish_b(0, 1)
    finish_x(0, 1)
    relay(1, 1)
    finish_a(1, 0)
    relay(1, 2)
    finish_b(1, 0)
    finish_x(1, 0)
    relay(1, 3)
    finish_a(1, 1)
    finish_b(1, 1)
    finish_x(1, 1)

    for s in range(series):
        partner_copy(s).wait_send()
        for h in range(2):
            x_copy(s, h, 1).wait_send()
        for r in range(PIECES):
            y_copy(s, r).wait_send()

    @pl.when(has_onward)
    def _():
        for s in range(series):
            for r in range(PIECES):
                z_copy(s, r).wait_send()


def attention_kernel(
    lengths_ref, window_ref, queries_ref, context_ref, out_ref, bias_ref, *, s, hops
):
    rows, width = out_ref.shape
    keys = context_ref.shape[1]
    head_size = width // HEADS
    sharing = BLOCK // head_size
    pairs = width // BLOCK
    reach = WINDOW // BLOCK
    parts = rows // BLOCK
    me = lax.axis_index("tm")
    patches = rows * lax.axis_size("tm")
    first = me * rows - hops * rows
    center = hops * rows // BLOCK
    start = patches - lengths_ref[s]
    key_pos = first + lax.broadcasted_iota(jnp.int32, (1, keys), 1)
    bias_ref[...] = jnp.where((key_pos >= start) & (key_pos < patches), 0.0, MASKED)
    query_valid = me * rows + lax.broadcasted_iota(jnp.int32, (rows, BLOCK), 0) >= start
    lane = lax.broadcasted_iota(jnp.int32, (rows, BLOCK), 1)
    tilt = lax.broadcasted_iota(jnp.int32, (BLOCK, BLOCK), 1) - lax.broadcasted_iota(
        jnp.int32, (BLOCK, BLOCK), 0
    )

    mine = [lane[:BLOCK] // head_size == h for h in range(sharing)]

    def one_head(pair, h, steps, window):
        column = pl.multiple_of(pair * BLOCK, BLOCK)
        span = (2 * steps + 1) * BLOCK
        for part in range(parts):
            low = (center + part - steps) * BLOCK
            q = queries_ref[s, part * BLOCK : (part + 1) * BLOCK, pl.ds(column, BLOCK)]
            q = jnp.where(mine[h], q, jnp.zeros_like(q))
            k = context_ref[s, low : low + span, pl.ds(column, BLOCK)]
            scores = lax.dot_general(
                q, k, (((1,), (1,)), ((), ())), preferred_element_type=jnp.float32
            )
            chunks = []
            for o in range(-steps, steps + 1):
                at = (o + steps) * BLOCK
                chunk = scores[:, at : at + BLOCK] + bias_ref[:, low + at : low + at + BLOCK]
                if abs(o) >= steps - 1:
                    if o <= 0:
                        chunk = jnp.where(tilt >= -(window + o * BLOCK), chunk, MASKED)
                    if o >= 0:
                        chunk = jnp.where(tilt <= window - o * BLOCK, chunk, MASKED)
                chunks.append(chunk)
            top = functools.reduce(jnp.maximum, chunks)
            top = jnp.max(top, axis=1, keepdims=True)
            weights = jnp.concatenate(
                [jnp.exp(chunk - top).astype(jnp.bfloat16) for chunk in chunks], axis=1
            )
            v = context_ref[s, low : low + span, pl.ds(width + column, BLOCK)]
            v = jnp.concatenate([v, jnp.ones((span, BLOCK), jnp.bfloat16)], axis=1)
            both = jnp.dot(weights, v, preferred_element_type=jnp.float32)
            result = both[:, :BLOCK] / both[:, BLOCK:]
            valid = query_valid[part * BLOCK : (part + 1) * BLOCK]
            result = jnp.where(valid, result, 0.0).astype(jnp.bfloat16)
            place = (slice(part * BLOCK, (part + 1) * BLOCK), pl.ds(column, BLOCK))
            if h:
                result = jnp.where(mine[h], result, out_ref[place])
            out_ref[place] = result

    def body(pair, _):
        for h in range(sharing):
            window = window_ref[pair * sharing + h]
            needed = (window + BLOCK - 1) // BLOCK
            for steps in range(1, reach + 1):
                @pl.when(needed == steps)
                def _():
                    one_head(pair, h, steps, window)
        return 0

    lax.fori_loop(0, pairs, body, 0)


def mixing_kernel(mix_ref, up_ref, *refs, series, groups):
    hiddens, parts, out_ref = refs[:series], refs[series:-1], refs[-1]
    group = lax.axis_index("series")
    for a in range(series):
        total = None
        for index, part in enumerate(parts):
            offset = index % groups
            column = lax.rem(group - offset + groups, groups) * series + index // groups
            term = mix_ref[group * series + a, column] * part[...].astype(jnp.float32)
            total = term if total is None else total + term
        update = jnp.dot(
            total.astype(jnp.bfloat16), up_ref[...], preferred_element_type=jnp.float32
        )
        out_ref[a] = (hiddens[a][...].astype(jnp.float32) + update).astype(jnp.bfloat16)


def on_device(
    history, lengths, head_window, input_proj, output_proj, mixer_down, mixer_up, series_mix
):
    series, rows, width = history.shape
    hops = -(-WINDOW // rows)
    keys = (2 * hops + 1) * rows
    head_size = width // HEADS
    vmem = pl.BlockSpec(memory_space=pltpu.VMEM)
    smem = pl.BlockSpec(memory_space=pltpu.SMEM)
    dma = pltpu.SemaphoreType.DMA
    queries, context = pl.pallas_call(
        functools.partial(exchange_kernel, scale=head_size ** (-0.5)),
        out_shape=(
            pltpu.VMEM((series, rows, width), jnp.bfloat16),
            pltpu.VMEM((series, keys, 2 * width), jnp.bfloat16),
        ),
        in_specs=[vmem, pl.BlockSpec(memory_space=pltpu.HBM)],
        out_specs=(vmem, vmem),
        scratch_shapes=[
            pltpu.VMEM((4, series, rows, width), jnp.bfloat16),
            pltpu.VMEM(input_proj.shape, jnp.bfloat16),
            dma((6,)),
            dma((series,)),
            dma((series,)),
            dma((series, PIECES)),
            dma((series, PIECES)),
            dma((series, PIECES)),
            dma((series, PIECES)),
            dma((series, 2)),
            dma((series, 2)),
        ],
        compiler_params=pltpu.CompilerParams(
            collective_id=0, has_side_effects=True, vmem_limit_bytes=LIMIT * 1024 * 1024
        ),
    )(history, input_proj)
    groups = lax.axis_size("series")
    mix = series_mix.astype(jnp.float32)
    hiddens = []
    parts = []
    for s in range(series):
        attended = pl.pallas_call(
            functools.partial(attention_kernel, s=s, hops=hops),
            out_shape=jax.ShapeDtypeStruct((rows, width), jnp.bfloat16),
            in_specs=[smem, smem, vmem, vmem],
            out_specs=vmem,
            scratch_shapes=[
                pltpu.VMEM((1, keys), jnp.float32),
            ],
            compiler_params=pltpu.CompilerParams(vmem_limit_bytes=32 * 1024 * 1024),
            cost_estimate=pl.CostEstimate(
                flops=8 * rows * keys * width, bytes_accessed=0, transcendentals=0
            ),
        )(lengths, head_window, queries, context)
        hidden = (
            history[s].astype(jnp.float32)
            + jnp.dot(attended, output_proj, preferred_element_type=jnp.float32)
        ).astype(jnp.bfloat16)
        hiddens.append(hidden)
        branch = jnp.dot(hidden, mixer_down, preferred_element_type=jnp.float32).astype(
            jnp.bfloat16
        )
        for offset in range(groups):
            route = [(i, (i + offset) % groups) for i in range(groups)]
            parts.append(lax.ppermute(branch, "series", route) if offset else branch)
    return pl.pallas_call(
        functools.partial(mixing_kernel, series=series, groups=groups),
        out_shape=jax.ShapeDtypeStruct(history.shape, jnp.bfloat16),
        in_specs=[smem, vmem] + [vmem] * (len(hiddens) + len(parts)),
        out_specs=vmem,
        compiler_params=pltpu.CompilerParams(vmem_limit_bytes=32 * 1024 * 1024),
    )(mix, mixer_up, *hiddens, *parts)


def solution(mesh):
    in_specs = (P("series", "tm", None), P("series"), P(), P(), P(), P(), P(), P())
    out_specs = P("series", "tm", None)
    return jax.shard_map(
        on_device, mesh=mesh, in_specs=in_specs, out_specs=out_specs, check_vma=False
    )
```
